32 devices in a mesh: section: 2 (over x), seq: 8 (over z, y), rep: 2 (over core).
Axes of the slice: x: 2, y: 2, z: 4, core: 2. Of those that a mesh axis runs over, the one named last changes fastest.
Arguments:
- queries: bfloat16 [512, 2560], P('seq', ('section', 'rep')), may hold values from -5 to 5
- keys: bfloat16 [512, 2560], P('seq', ('section', 'rep')), may hold values from -5 to 5
- values: bfloat16 [512, 2560], P('seq', ('section', 'rep')), may hold values from -6 to 6
- block_order: int32 [16], replicated, may hold values from 0 to 15, each once
- wo: bfloat16 [2560, 5120], P(('section', 'rep'), 'seq'), may hold values from -0.125 to 0.125
- resid: bfloat16 [4, 5120, 128], P(('section', 'rep'), 'seq'), may hold values from -60 to 60
- gain: bfloat16 [5120], P('seq'), may hold values from 0.099609375 to 1.8984375
- w_gate: bfloat16 [13824, 5120], P('seq'), may hold values from -0.078125 to 0.078125
- w_up: bfloat16 [13824, 5120], P('seq'), may hold values from -0.078125 to 0.078125
- w_down: bfloat16 [13824, 5120], P('seq'), may hold values from -0.0625 to 0.0625
Outputs:
- mixed: bfloat16 [4, 5120, 128], P(('section', 'rep'), 'seq')
The draws below stay inside these ranges and needn't reach their ends.
Inputs may be any that keep to these rules, and one draw needn't show every extreme that they name: `block_order`: each number once.
All inputs are finite; a program needn't handle non-finite values.
Results may differ from the reference program's by a relative error of at most 0.0055.
Values may be sent and summed in bfloat16 or wider, within the bound.
No kernel may reach another device: no remote copies, remote signals or barrier semaphores. Data moves between devices by JAX's collectives and lax.ppermute only.
A program may use at most 128 MiB of HBM per device.

```python
import jax
import jax.numpy as jnp
from jax import lax

D = 5120
FF = 13824
HEADS = 20
HEAD_DIM = 128
SEQ_DEV = 64
TOKENS = 512
HW = 2560
GROUPS = 4
SUB = 16
BLOCKS = 16
N_SEQ = 8


def query_key_pair(key):
    queries = jnp.clip(jax.random.normal(jax.random.fold_in(key, 11), (TOKENS, HW), jnp.float32), -5.0, 5.0)
    keys = jnp.clip(jax.random.normal(jax.random.fold_in(key, 12), (TOKENS, HW), jnp.float32), -5.0, 5.0)
    return (queries, keys)


def draw_queries(key, part):
    return query_key_pair(key)[0].astype(jnp.bfloat16)


def draw_keys(key, part):
    return query_key_pair(key)[1].astype(jnp.bfloat16)


def draw_resid(key, part):
    base = jnp.clip(jax.random.normal(jax.random.fold_in(key, 21), (GROUPS, D, N_SEQ * SUB), jnp.float32), -6.0, 6.0)
    rising = (3.0 ** (jnp.arange(D, dtype=jnp.float32) / D)).reshape(1, D, 1)
    return jnp.clip(base * rising, -60.0, 60.0).astype(jnp.bfloat16)


def raised(entries, rng, source, target, blocks, factor):
    def block_of(axis_at):
        return (jnp.arange(entries.shape[axis_at]) // (entries.shape[axis_at] // blocks)).reshape((-1,) + (1,) * (entries.ndim - 1 - axis_at))

    one_side = jax.random.permutation(rng, blocks)[block_of(target)]
    second = (block_of(target) + blocks // 2) % blocks
    return jnp.where((block_of(source) == one_side) | (block_of(source) == second), factor * entries, entries)


def shard_levels(stream_key, dims, pieces, least, top_value):
    loudness = 1.0
    for position, parts in pieces:
        draws = jax.random.uniform(jax.random.fold_in(jax.random.fold_in(stream_key, 6), position), (parts,), jnp.float32, least / len(pieces), top_value / len(pieces))
        loudness = loudness * jnp.repeat(jnp.exp(draws), dims[position] // parts).reshape((-1,) + (1,) * (len(dims) - 1 - position))
    return loudness


def gaussian(rng, dims, spread, bound, shards=(), held_as=jnp.bfloat16):
    level = shard_levels(rng, dims, shards, -0.22, 0.18) if shards else 1.0
    result = jax.random.normal(rng, dims, jnp.float32) * spread * level
    return jnp.minimum(jnp.maximum(result, -bound), bound).astype(held_as)


def heavy_noise(own_key, shape, scale, limit, pieces, heavy, kind=jnp.bfloat16):
    values = scale * jax.random.normal(own_key, shape, jnp.float32)
    if pieces:
        values = values * shard_levels(own_key, shape, pieces, -0.22, 0.18)
    return jnp.clip(raised(values, jax.random.fold_in(own_key, 3), *heavy), -limit, limit).astype(kind)


def setup_inputs(seed: int = 0) -> dict:
    key_of = jax.random.split(jax.random.key(seed), 11)
    return {
        "queries": draw_queries(jax.random.fold_in(key_of[10], 71), 0),
        "keys": draw_keys(jax.random.fold_in(key_of[10], 71), 0),
        "values": gaussian(key_of[2], (TOKENS, HW), 1.0, 6.0, ((0, 8), (1, 4))),
        "block_order": jax.random.permutation(key_of[3], BLOCKS).astype(jnp.int32),
        "wo": gaussian(key_of[4], (HW, D), HW ** -0.5, 0.125, ((0, 4), (1, 8))),
        "resid": draw_resid(jax.random.fold_in(key_of[10], 71), 0),
        "gain": jnp.clip(1.0 + 0.18 * jax.random.normal(key_of[6], (D,), jnp.float32), 0.099609375, 1.8984375).astype(jnp.bfloat16),
        "w_gate": gaussian(key_of[7], (FF, D), D ** -0.5, 0.078125, ((0, 8),)),
        "w_up": gaussian(key_of[8], (FF, D), D ** -0.5, 0.078125, ((0, 8),)),
        "w_down": heavy_noise(key_of[9], (FF, D), FF ** -0.5, 0.0625, ((0, 8),), (0, 1, 8, 2.0)),
    }


def reference(queries, keys, values, block_order, wo, resid, gain, w_gate, w_up, w_down):
    block_rows = SEQ_DEV // 2
    row_ids = jnp.arange(TOKENS, dtype=jnp.int32)
    pos = block_order[row_ids // block_rows].astype(jnp.int32) * block_rows + row_ids % block_rows
    visible = pos[None, :] <= pos[:, None]
    scale = HEAD_DIM ** (-0.5)
    query_heads = queries.reshape(TOKENS, HEADS, HEAD_DIM).transpose(1, 0, 2)
    key_heads = keys.reshape(TOKENS, HEADS, HEAD_DIM).transpose(1, 0, 2)
    value_heads = values.reshape(TOKENS, HEADS, HEAD_DIM).transpose(1, 0, 2)

    def one_head(operands):
        q_head, k_head, v_head = operands
        scores = jnp.dot(q_head, k_head.T, preferred_element_type=jnp.float32) * scale
        scores = jnp.where(visible, scores, -jnp.inf)
        top = lax.optimization_barrier(jnp.max(scores, axis=-1, keepdims=True))
        probs = jnp.exp(scores - top)
        total = lax.optimization_barrier(jnp.sum(probs, axis=-1, keepdims=True))
        out = jnp.dot(probs.astype(jnp.bfloat16), v_head, preferred_element_type=jnp.float32) / total
        return out.astype(jnp.bfloat16)
    attended = lax.map(one_head, (query_heads, key_heads, value_heads))
    attended = attended.transpose(1, 0, 2).reshape(TOKENS, HW)
    resid_rows = resid.reshape(GROUPS, D, N_SEQ, SUB).transpose(2, 0, 3, 1).reshape(TOKENS, D)
    carried = resid_rows.astype(jnp.float32) + jnp.dot(attended, wo, preferred_element_type=jnp.float32)
    meansq = lax.optimization_barrier(jnp.mean(carried * carried, axis=-1, keepdims=True))
    normed = (carried * lax.rsqrt(meansq + 1e-05) * gain.astype(jnp.float32)).astype(jnp.bfloat16)
    gate = jnp.dot(normed, w_gate.T, preferred_element_type=jnp.float32)
    up = jnp.dot(normed, w_up.T, preferred_element_type=jnp.float32)
    hidden = (jax.nn.silu(gate) * up).astype(jnp.bfloat16)
    down = jnp.dot(hidden, w_down, preferred_element_type=jnp.float32)
    mixed = (carried + down).astype(jnp.bfloat16)
    return mixed.reshape(N_SEQ, GROUPS, SUB, D).transpose(1, 3, 0, 2).reshape(GROUPS, D, N_SEQ * SUB)
```

```python
import math

import jax
import jax.numpy as jnp
from jax import lax
from jax.experimental import pallas as pl
from jax.experimental.pallas import tpu as pltpu
from jax.sharding import PartitionSpec as P

D = 5120
HEAD_DIM = 128
EPS = 1e-05
LOG2E = 1.4426950408889634
MIB = 1 << 20
FETCH_FLOPS = 300
VMEM = pl.BlockSpec(memory_space=pltpu.VMEM)
HBM = pl.BlockSpec(memory_space=pltpu.MemorySpace.HBM)
SMEM = pl.BlockSpec(memory_space=pltpu.SMEM)


def key_positions(order, start, count, block_rows):
    row_ids = start + jnp.arange(count, dtype=jnp.int32)
    owners = row_ids // block_rows
    match = owners[:, None] == jnp.arange(order.shape[0], dtype=jnp.int32)[None, :]
    first = jnp.sum(jnp.where(match, order[None, :], 0), axis=1)
    return first * block_rows + row_ids % block_rows


def gathered(queries, keys, values, block_order, wo, resid, gain, w_gate, w_up, w_down):
    seq_dev = queries.shape[0]
    heads_dev = queries.shape[1] // HEAD_DIM
    groups = lax.axis_size("section") * lax.axis_size("rep")
    n_seq = lax.axis_size("seq")
    sub_rows = seq_dev // groups
    block_rows = seq_dev // 2
    query_start = lax.axis_index("seq") * seq_dev
    query_pos = key_positions(block_order, query_start, seq_dev, block_rows)
    query_heads = queries.reshape(seq_dev, heads_dev, HEAD_DIM)
    scale = HEAD_DIM ** (-0.5)
    running_max = jnp.full((seq_dev, heads_dev), -1e30, jnp.float32)
    key_piece = lax.all_gather(keys, "seq", axis=0, tiled=True)
    value_piece = lax.all_gather(values, "seq", axis=0, tiled=True)
    count = key_piece.shape[0]
    key_pos = key_positions(block_order, jnp.int32(0), count, block_rows)
    scores = (
        jnp.einsum(
            "qhd,khd->qhk",
            query_heads,
            key_piece.reshape(count, heads_dev, HEAD_DIM),
            preferred_element_type=jnp.float32,
        )
        * scale
    )
    visible = (key_pos[None, :] <= query_pos[:, None])[:, None, :]
    new_max = jnp.maximum(running_max, jnp.max(jnp.where(visible, scores, -1e30), axis=-1))
    probs = jnp.where(visible, jnp.exp(scores - new_max[..., None]), 0.0)
    total = jnp.sum(probs, axis=-1)
    weighted = jnp.einsum(
        "qhk,khd->qhd",
        probs.astype(jnp.bfloat16),
        value_piece.reshape(count, heads_dev, HEAD_DIM),
        preferred_element_type=jnp.float32,
    )
    running_max, total, weighted = (new_max, total, weighted)
    attended = (
        (weighted / total[..., None]).astype(jnp.bfloat16).reshape(seq_dev, heads_dev * HEAD_DIM)
    )
    columns = wo.shape[1]
    token_count = n_seq * sub_rows
    parts = attended.reshape(groups, sub_rows, heads_dev * HEAD_DIM)
    group_rows = lax.all_to_all(parts, ("section", "rep"), split_axis=0, concat_axis=2, tiled=True)
    wo_columns = lax.all_gather(wo, ("section", "rep"), axis=0, tiled=True)
    piece = lax.all_gather(group_rows, "seq", axis=0, tiled=True)
    flat = piece.reshape(piece.shape[0] * piece.shape[1], piece.shape[2])
    product = jnp.dot(flat, wo_columns, preferred_element_type=jnp.float32)
    projected = product.reshape(piece.shape[0], piece.shape[1], columns)
    projected_cols = projected.reshape(token_count, columns).T
    carried = resid.reshape(columns, token_count).astype(jnp.float32) + projected_cols
    squares = lax.psum(jnp.sum(carried * carried, axis=0), "seq")
    normed = (
        carried * lax.rsqrt(squares / D + 1e-05)[None, :] * gain.astype(jnp.float32)[:, None]
    ).astype(jnp.bfloat16)
    piece = lax.all_gather(normed, "seq", axis=0, tiled=True)
    gate_sum = jnp.dot(w_gate, piece, preferred_element_type=jnp.float32)
    up_sum = jnp.dot(w_up, piece, preferred_element_type=jnp.float32)
    hidden = (jax.nn.silu(gate_sum) * up_sum).astype(jnp.bfloat16)
    term = lax.dot_general(
        w_down, hidden, (((0,), (0,)), ((), ())), preferred_element_type=jnp.float32
    )
    down = lax.psum_scatter(term, "seq", scatter_dimension=0, tiled=True)
    return (carried + down).astype(jnp.bfloat16).reshape(resid.shape)


def call(body, outs, args, scalars=0, scratch=(), limit=7, flops=0, nbytes=0, aliases=None, in_place=()):
    spaces = [SMEM] * scalars + [VMEM] * (len(args) - scalars)
    for i in in_place:
        spaces[i] = HBM
    return pl.pallas_call(
        body,
        out_shape=outs,
        in_specs=spaces,
        out_specs=jax.tree.map(lambda _: VMEM, outs),
        scratch_shapes=list(scratch),
        input_output_aliases=aliases or {},
        compiler_params=pltpu.CompilerParams(vmem_limit_bytes=limit * MIB),
        cost_estimate=pl.CostEstimate(flops=flops, bytes_accessed=nbytes, transcendentals=0),
    )(*args)


def struct(shape, dtype):
    return jax.ShapeDtypeStruct(shape, dtype)


def swap(x, offset, n_seq):
    return lax.ppermute(x, "seq", [(i, i ^ offset) for i in range(n_seq)])


def gather(x, n_seq):
    got = {4: swap(x, 4, n_seq), 2: swap(x, 2, n_seq), 1: swap(x, 1, n_seq)}
    got[6] = swap(got[4], 2, n_seq)
    for r in (2, 4, 6):
        got[r + 1] = swap(got[r], 1, n_seq)
    return [x] + [got[r] for r in range(1, n_seq)]


def in_hbm(x):
    return pltpu.with_memory_space_constraint(x, pltpu.MemorySpace.HBM)


def fetch(arrays, outs):
    def body(*refs):
        ins, refs = refs[: len(arrays)], refs[len(arrays) :]
        tiles, sems = refs[:-1], refs[-1]
        rows_of = [(ref, k) for ref in ins for k in range(ref.shape[0] // step)]
        spots = [(tile, k) for tile in tiles for k in range(tile.shape[0] // step)]
        copies = [
            pltpu.make_async_copy(a.at[pl.ds(i * step, step)], b.at[pl.ds(k * step, step)], sems.at[n])
            for n, ((a, i), (b, k)) in enumerate(zip(rows_of, spots))
        ]
        for c in copies:
            c.start()
        for c in copies:
            c.wait()

    step = math.gcd(*outs, *(a.shape[0] for a in arrays))
    width, dtype = arrays[0].shape[1], arrays[0].dtype
    nbytes = 2 * sum(outs) * width
    return pl.pallas_call(
        body,
        out_shape=[pltpu.VMEM((rows, width), dtype) for rows in outs],
        in_specs=[HBM] * len(arrays),
        out_specs=[VMEM] * len(outs),
        scratch_shapes=[pltpu.SemaphoreType.DMA((sum(outs) // step,))],
        compiler_params=pltpu.CompilerParams(vmem_limit_bytes=MIB),
        cost_estimate=pl.CostEstimate(flops=FETCH_FLOPS * nbytes, bytes_accessed=nbytes, transcendentals=0),
    )(*(in_hbm(a) for a in arrays))


def attend_body(n_seq, seq_dev, heads_dev, groups, reps):
    sub = seq_dev // groups
    half = seq_dev // 2
    tokens = n_seq * seq_dev
    per_group = n_seq * sub

    def body(place, *refs):
        blocks, wo_t, send, keep, att = refs[:n_seq], *refs[n_seq:]
        me, section, rep = place[0], place[1], place[2]
        lane = lax.broadcasted_iota(jnp.int32, (1, tokens), 1)
        row = lax.broadcasted_iota(jnp.int32, (seq_dev, 1), 0)
        key_pos = jnp.zeros((1, tokens), jnp.int32)
        query_pos = []
        for r in range(n_seq):
            source = me ^ r
            low, high = place[3 + 2 * source] * half, place[4 + 2 * source] * half
            key_pos = jnp.where(lane >= r * seq_dev, low + lane - r * seq_dev, key_pos)
            key_pos = jnp.where(lane >= r * seq_dev + half, high + lane - r * seq_dev - half, key_pos)
            query_pos.append(jnp.where(row < half, low + row, high + row - half))
        query_pos = jnp.concatenate(query_pos, axis=0)
        for h in range(heads_dev):
            cols = pl.ds(h * HEAD_DIM, HEAD_DIM)
            q, k, v = (
                jnp.concatenate([b[pl.ds(i * seq_dev, seq_dev), cols] for b in blocks], axis=0)
                for i in range(3)
            )
            scores = lax.dot_general(q, k, (((1,), (1,)), ((), ())), preferred_element_type=jnp.float32)
            scores = jnp.where(key_pos <= query_pos, scores, -1e30)
            top = jnp.max(scores, axis=-1, keepdims=True)
            probs = jnp.exp2((scores - top) * (HEAD_DIM**-0.5 * LOG2E))
            total = jnp.sum(probs, axis=-1, keepdims=True)
            out = jnp.dot(probs.astype(jnp.bfloat16), v, preferred_element_type=jnp.float32)
            out = (out / total).astype(jnp.bfloat16)
            for r in range(n_seq):
                source = me ^ r
                for g in range(groups):
                    slot = ((g % reps) ^ rep) * (groups // reps) + ((g // reps) ^ section)
                    start = pl.multiple_of(slot * per_group + source * sub, sub)
                    at = r * seq_dev + g * sub
                    att[pl.ds(start, sub), cols] = out[at : at + sub]
        product = lax.dot_general(
            wo_t[...], att[...], (((1,), (1,)), ((), ())), preferred_element_type=jnp.float32
        )
        keep[...] = product[:, : tokens // 2]
        send[...] = product[:, tokens // 2 :].astype(jnp.bfloat16)

    return body


def halve_body(keep, got, send, rest):
    half = rest.shape[1]
    rest[...] = keep[:, :half] + got[:, :half].astype(jnp.float32)
    send[...] = (keep[:, half:] + got[:, half:].astype(jnp.float32)).astype(jnp.bfloat16)


def carry_body(rest, got, resid, gain, carried, out):
    columns = rest.shape[0]
    total = rest[...] + got[...].astype(jnp.float32) + resid[...].astype(jnp.float32)
    carried[...] = total
    squares = jnp.sum(total * total, axis=0, keepdims=True)
    high = squares.astype(jnp.bfloat16)
    low = (squares - high.astype(jnp.float32)).astype(jnp.bfloat16)
    pick = lax.broadcasted_iota(jnp.int32, (16, total.shape[1]), 0)
    both = jnp.where(pick == 0, high.astype(jnp.float32), jnp.where(pick == 1, low.astype(jnp.float32), 0.0))
    out[pl.ds(0, columns), :] = (total * gain[...]).astype(jnp.bfloat16)
    out[pl.ds(columns, 16), :] = both.astype(jnp.bfloat16)


def row_tile(rows):
    return max(t for t in range(16, 601, 16) if rows % t == 0)


def gate_body(offsets, columns, tiles, first, last):
    n = len(offsets)

    def body(place, *refs):
        xs, refs = refs[:n], refs[n:]
        weights, refs = (refs[: len(tiles)], refs[len(tiles) : 2 * len(tiles)]), refs[2 * len(tiles) :]
        sums, refs = (None, refs) if first else (refs[:3], refs[3:])
        spots = [pl.ds(pl.multiple_of((place[0] ^ r) * columns, 128), columns) for r in offsets]
        squares = [jnp.sum(x[pl.ds(columns, 16), :].astype(jnp.float32), axis=0, keepdims=True) for x in xs]
        squares = sum(squares[1:], squares[0])
        if not first:
            squares = squares + sums[2][pl.ds(0, 1), :]
        scale = lax.rsqrt(squares / D + EPS) if last else None
        for i, tile in enumerate(tiles):
            rows = pl.ds(sum(tiles[:i]), tile)
            products = []
            for j, weight in enumerate(weights):
                total = None if first else sums[j][rows, :]
                for x, at in zip(xs, spots):
                    part = jnp.dot(weight[i][:, at], x[pl.ds(0, columns), :], preferred_element_type=jnp.float32)
                    total = part if total is None else total + part
                products.append(total)
            if last:
                gate, up = products[0] * scale, products[1] * scale
                refs[1][rows, :] = gate / (1.0 + jnp.exp(-gate)) * up
            else:
                refs[0][rows, :], refs[1][rows, :] = products
        if last:
            refs[0][...] = refs[1][...].T.astype(jnp.bfloat16)
        else:
            refs[2][...] = jnp.broadcast_to(squares, refs[2].shape)

    return body


def down_body(offsets, columns, tiles):
    def body(place, hidden, *refs):
        weights, outs = refs[: len(tiles)], refs[len(tiles) :]
        for r, out in zip(offsets, outs):
            at = pl.ds(pl.multiple_of((place[0] ^ r) * columns, 128), columns)
            total = None
            for i, tile in enumerate(tiles):
                part = jnp.dot(hidden[:, sum(tiles[:i]) : sum(tiles[: i + 1])], weights[i][:, at], preferred_element_type=jnp.float32)
                total = part if total is None else total + part
            out[...] = total.astype(out.dtype)

    return body


def add_body(mine, got, out):
    out[...] = (mine[...].astype(jnp.float32) + got[...].astype(jnp.float32)).astype(out.dtype)


def finish_body(carried, mine, *refs):
    total = mine[...]
    for got in refs[:-1]:
        total = total + got[...].astype(jnp.float32)
    refs[-1][...] = (carried[...] + total.T).astype(jnp.bfloat16)


def exchanged(queries, keys, values, block_order, wo, resid, gain, w_gate, w_up, w_down):
    f32, bf16 = jnp.float32, jnp.bfloat16
    seq_dev, heads_features = queries.shape
    n_seq, reps = lax.axis_size("seq"), lax.axis_size("rep")
    groups = lax.axis_size("section") * reps
    tokens = n_seq * seq_dev
    group_tokens = tokens // groups
    columns = wo.shape[1]
    units = w_gate.shape[0]
    place = jnp.stack([lax.axis_index(a).astype(jnp.int32) for a in ("seq", "section", "rep")])
    place = jnp.concatenate([place, block_order])

    blocks = gather(fetch([queries, keys, values], [3 * seq_dev])[0], n_seq)
    tile = row_tile(units)
    tiles = [tile] * (units // tile)
    w_gate, w_up, w_down = (fetch([w], tiles) for w in (w_gate, w_up, w_down))
    send, keep = call(
        attend_body(n_seq, seq_dev, heads_features // HEAD_DIM, groups, reps),
        (struct((columns, tokens // 2), bf16), struct((columns, tokens // 2), f32)),
        (place, *blocks, wo.T),
        scalars=1,
        scratch=[pltpu.VMEM((tokens, heads_features), bf16)],
        limit=7,
        flops=6 * 10**9,
    )
    got = lax.ppermute(send, "rep", [(0, 1), (1, 0)])
    send, rest = call(
        halve_body, (struct((columns, group_tokens), bf16), struct((columns, group_tokens), f32)), (keep, got), limit=3
    )
    got = lax.ppermute(send, "section", [(0, 1), (1, 0)])
    gain_wide = jnp.broadcast_to(gain.astype(f32)[:, None], (columns, group_tokens))
    carried, x = call(
        carry_body,
        (struct((columns, group_tokens), f32), struct((columns + 16, group_tokens), bf16)),
        (rest, got, resid.reshape(columns, group_tokens), gain_wide),
        limit=3,
    )
    xs = gather(x, n_seq)
    acc = ()
    shares = ((0, 1, 2), (3, 4), (6, 5), (7,))
    for i, share in enumerate(shares):
        last = i == len(shares) - 1
        n = len(share)
        if last:
            outs = struct((group_tokens, units), bf16)
        else:
            outs = (struct((units, group_tokens), f32),) * 2 + (struct((8, group_tokens), f32),)
        acc = call(
            gate_body(share, columns, tiles, i == 0, last),
            outs,
            (place, *(xs[r] for r in share), *w_gate, *w_up, *acc),
            scalars=1,
            scratch=[pltpu.VMEM((units, group_tokens), f32)] if last else [],
            limit=4,
            flops=4 * units * columns * group_tokens * n,
            aliases={} if last or i == 0 else {1 + n + 2 * len(tiles) + j: j for j in range(3)},
        )
    hidden = acc

    def down(*offsets_types):
        return call(
            down_body([r for r, _ in offsets_types], columns, tiles),
            tuple(struct((group_tokens, columns), t) for _, t in offsets_types),
            (place, hidden, *w_down),
            scalars=1,
            limit=3,
            flops=2 * units * columns * group_tokens * len(offsets_types),
        )

    def plus(mine, got):
        return call(add_body, struct((group_tokens, columns), bf16), (mine, got), limit=3)

    own, far = {}, {}
    far[6], = down((7, bf16))
    own[6], far[4] = down((6, f32), (5, bf16))
    own[4], far[2] = down((4, f32), (3, bf16))
    own[2], far[0], own[0] = down((2, f32), (1, bf16), (0, f32))
    got = {r: swap(far[r], 1, n_seq) for r in (6, 4, 2, 0)}
    sums = {6: plus(own[6], got[6])}
    onward = swap(sums[6], 2, n_seq)
    sums[2] = plus(own[2], got[2])
    sums[4] = plus(plus(own[4], got[4]), onward)
    parts = [got[0], swap(sums[2], 2, n_seq), swap(sums[4], 4, n_seq)]
    out = call(finish_body, struct((columns, group_tokens), bf16), (carried, own[0], *parts), limit=3)
    return out.reshape(resid.shape)


def on_device(queries, keys, values, block_order, wo, resid, gain, w_gate, w_up, w_down):
    groups = lax.axis_size("section") * lax.axis_size("rep")
    n_seq = lax.axis_size("seq")
    fits = (
        n_seq == 8
        and groups == 4
        and lax.axis_size("rep") == 2
        and wo.shape[1] % 128 == 0
        and (queries.shape[0] // groups) % 16 == 0
        and (queries.shape[0] * n_seq // groups) % 128 == 0
    )
    form = exchanged if fits else gathered
    return form(queries, keys, values, block_order, wo, resid, gain, w_gate, w_up, w_down)


def solution(mesh):
    return jax.shard_map(
        on_device,
        mesh=mesh,
        in_specs=(
            P("seq", ("section", "rep")),
            P("seq", ("section", "rep")),
            P("seq", ("section", "rep")),
            P(),
            P(("section", "rep"), "seq"),
            P(("section", "rep"), "seq", None),
            P("seq"),
            P("seq", None),
            P("seq", None),
            P("seq", None),
        ),
        out_specs=P(("section", "rep"), "seq", None),
        check_vma=False,
    )
```

```python
import jax
import jax.numpy as jnp
from jax import lax
from jax.experimental import pallas as pl
from jax.experimental.pallas import tpu as pltpu
from jax.sharding import PartitionSpec as P


D = 5120
HEAD_DIM = 128
EPS = 1e-05
LOG2E = 1.4426950408889634
MIB = 1 << 20
SEQ = 8
SHARES = ((0, 1), (2, 4), (5, 6), (3, 7))
VMEM = pl.BlockSpec(memory_space=pltpu.VMEM)
HBM = pl.BlockSpec(memory_space=pltpu.MemorySpace.HBM)
SMEM = pl.BlockSpec(memory_space=pltpu.SMEM)


def key_positions(order, start, count, block_rows):
    row_ids = start + jnp.arange(count, dtype=jnp.int32)
    owners = row_ids // block_rows
    match = owners[:, None] == jnp.arange(order.shape[0], dtype=jnp.int32)[None, :]
    first = jnp.sum(jnp.where(match, order[None, :], 0), axis=1)
    return first * block_rows + row_ids % block_rows


def gathered(queries, keys, values, block_order, wo, resid, gain, w_gate, w_up, w_down):
    seq_dev = queries.shape[0]
    heads_dev = queries.shape[1] // HEAD_DIM
    groups = lax.axis_size("section") * lax.axis_size("rep")
    n_seq = lax.axis_size("seq")
    sub_rows = seq_dev // groups
    block_rows = seq_dev // 2
    query_start = lax.axis_index("seq") * seq_dev
    query_pos = key_positions(block_order, query_start, seq_dev, block_rows)
    query_heads = queries.reshape(seq_dev, heads_dev, HEAD_DIM)
    scale = HEAD_DIM ** (-0.5)
    running_max = jnp.full((seq_dev, heads_dev), -1e30, jnp.float32)
    key_piece = lax.all_gather(keys, "seq", axis=0, tiled=True)
    value_piece = lax.all_gather(values, "seq", axis=0, tiled=True)
    count = key_piece.shape[0]
    key_pos = key_positions(block_order, jnp.int32(0), count, block_rows)
    scores = (
        jnp.einsum(
            "qhd,khd->qhk",
            query_heads,
            key_piece.reshape(count, heads_dev, HEAD_DIM),
            preferred_element_type=jnp.float32,
        )
        * scale
    )
    visible = (key_pos[None, :] <= query_pos[:, None])[:, None, :]
    new_max = jnp.maximum(running_max, jnp.max(jnp.where(visible, scores, -1e30), axis=-1))
    probs = jnp.where(visible, jnp.exp(scores - new_max[..., None]), 0.0)
    total = jnp.sum(probs, axis=-1)
    weighted = jnp.einsum(
        "qhk,khd->qhd",
        probs.astype(jnp.bfloat16),
        value_piece.reshape(count, heads_dev, HEAD_DIM),
        preferred_element_type=jnp.float32,
    )
    running_max, total, weighted = (new_max, total, weighted)
    attended = (
        (weighted / total[..., None]).astype(jnp.bfloat16).reshape(seq_dev, heads_dev * HEAD_DIM)
    )
    columns = wo.shape[1]
    token_count = n_seq * sub_rows
    parts = attended.reshape(groups, sub_rows, heads_dev * HEAD_DIM)
    group_rows = lax.all_to_all(parts, ("section", "rep"), split_axis=0, concat_axis=2, tiled=True)
    wo_columns = lax.all_gather(wo, ("section", "rep"), axis=0, tiled=True)
    piece = lax.all_gather(group_rows, "seq", axis=0, tiled=True)
    flat = piece.reshape(piece.shape[0] * piece.shape[1], piece.shape[2])
    product = jnp.dot(flat, wo_columns, preferred_element_type=jnp.float32)
    projected = product.reshape(piece.shape[0], piece.shape[1], columns)
    projected_cols = projected.reshape(token_count, columns).T
    carried = resid.reshape(columns, token_count).astype(jnp.float32) + projected_cols
    squares = lax.psum(jnp.sum(carried * carried, axis=0), "seq")
    normed = (
        carried * lax.rsqrt(squares / D + 1e-05)[None, :] * gain.astype(jnp.float32)[:, None]
    ).astype(jnp.bfloat16)
    piece = lax.all_gather(normed, "seq", axis=0, tiled=True)
    gate_sum = jnp.dot(w_gate, piece, preferred_element_type=jnp.float32)
    up_sum = jnp.dot(w_up, piece, preferred_element_type=jnp.float32)
    hidden = (jax.nn.silu(gate_sum) * up_sum).astype(jnp.bfloat16)
    term = lax.dot_general(
        w_down, hidden, (((0,), (0,)), ((), ())), preferred_element_type=jnp.float32
    )
    down = lax.psum_scatter(term, "seq", scatter_dimension=0, tiled=True)
    return (carried + down).astype(jnp.bfloat16).reshape(resid.shape)


def call(body, outs, args, scalars=0, scratch=(), limit=7, aliases=None, in_place=()):
    spaces = [SMEM] * scalars + [VMEM] * (len(args) - scalars)
    for i in in_place:
        spaces[i] = HBM
    return pl.pallas_call(
        body,
        out_shape=outs,
        in_specs=spaces,
        out_specs=jax.tree.map(lambda _: VMEM, outs),
        scratch_shapes=list(scratch),
        input_output_aliases=aliases or {},
        compiler_params=pltpu.CompilerParams(vmem_limit_bytes=limit * MIB),
        cost_estimate=pl.CostEstimate(flops=0, bytes_accessed=0, transcendentals=0),
    )(*args)


def struct(shape, dtype):
    return jax.ShapeDtypeStruct(shape, dtype)


def swap(x, offset, n_seq):
    return lax.ppermute(x, "seq", [(i, i ^ offset) for i in range(n_seq)])


def gather(x, n_seq):
    got = {r: swap(x, r, n_seq) for r in (4, 1, 2)}
    for r, source, offset in ((5, 4, 1), (6, 4, 2), (3, 2, 1), (7, 5, 2)):
        got[r] = swap(got[source], offset, n_seq)
    return [x] + [got[r] for r in range(1, n_seq)]


def in_hbm(x):
    return pltpu.with_memory_space_constraint(x, pltpu.MemorySpace.HBM)


def fetch(place, arrays, rows, bases):
    n, width = len(arrays), arrays[0].shape[1]

    def body(place, *refs):
        ins, out, sems = refs[:n], refs[n], refs[n + 1]
        copies = []
        for i, (source, base) in enumerate(zip(ins, bases)):
            start = pl.multiple_of(base(place), 16)
            copies.append(pltpu.make_async_copy(source.at[pl.ds(start, rows)], out.at[pl.ds(i * rows, rows)], sems.at[i]))
        for c in copies:
            c.start()
        for c in copies:
            c.wait()

    return pl.pallas_call(
        body,
        out_shape=pltpu.VMEM((n * rows, width), arrays[0].dtype),
        in_specs=[SMEM] + [HBM] * n,
        out_specs=VMEM,
        scratch_shapes=[pltpu.SemaphoreType.DMA((n,))],
        compiler_params=pltpu.CompilerParams(vmem_limit_bytes=MIB),
    )(place, *(in_hbm(a) for a in arrays))


def stack(arrays):
    rows, width = arrays[0].shape

    def body(*refs):
        ins, out, sems = refs[:-2], refs[-2], refs[-1]
        copies = [pltpu.make_async_copy(ref, out.at[pl.ds(i * rows, rows)], sems.at[i]) for i, ref in enumerate(ins)]
        for c in copies:
            c.start()
        for c in copies:
            c.wait()

    n = len(arrays)
    return pl.pallas_call(
        body,
        name="stack",
        out_shape=pltpu.VMEM((n * rows, width), arrays[0].dtype),
        in_specs=[HBM] * n,
        out_specs=VMEM,
        scratch_shapes=[pltpu.SemaphoreType.DMA((n,))],
        compiler_params=pltpu.CompilerParams(vmem_limit_bytes=MIB),
    )(*(in_hbm(a) for a in arrays))


def attend_body(n_seq, seq_dev, heads_dev, groups, reps):
    sub = seq_dev // groups
    half = seq_dev // 2
    tokens = n_seq * seq_dev
    per_group = n_seq * sub

    def body(place, *refs):
        blocks, wo_t, send, keep, att = refs[:n_seq], *refs[n_seq:]
        me, section, rep = place[0], place[1], place[2]
        lane = lax.broadcasted_iota(jnp.int32, (1, tokens), 1)
        row = lax.broadcasted_iota(jnp.int32, (seq_dev, 1), 0)
        key_pos = jnp.zeros((1, tokens), jnp.int32)
        query_pos = []
        for r in range(n_seq):
            source = me ^ r
            low, high = place[3 + 2 * source] * half, place[4 + 2 * source] * half
            key_pos = jnp.where(lane >= r * seq_dev, low + lane - r * seq_dev, key_pos)
            key_pos = jnp.where(lane >= r * seq_dev + half, high + lane - r * seq_dev - half, key_pos)
            query_pos.append(jnp.where(row < half, low + row, high + row - half))
        query_pos = jnp.concatenate(query_pos, axis=0)
        for h in range(heads_dev):
            cols = pl.ds(h * HEAD_DIM, HEAD_DIM)
            q, k, v = (
                jnp.concatenate([b[pl.ds(i * seq_dev, seq_dev), cols] for b in blocks], axis=0)
                for i in range(3)
            )
            scores = lax.dot_general(q, k, (((1,), (1,)), ((), ())), preferred_element_type=jnp.float32)
            scores = jnp.where(key_pos <= query_pos, scores, -1e30)
            top = jnp.max(scores, axis=-1, keepdims=True)
            probs = jnp.exp2((scores - top) * (HEAD_DIM**-0.5 * LOG2E))
            total = jnp.sum(probs, axis=-1, keepdims=True)
            out = jnp.dot(probs.astype(jnp.bfloat16), v, preferred_element_type=jnp.float32)
            out = (out / total).astype(jnp.bfloat16)
            for r in range(n_seq):
                source = me ^ r
                for g in range(groups):
                    slot = ((g % reps) ^ rep) * (groups // reps) + ((g // reps) ^ section)
                    start = pl.multiple_of(slot * per_group + source * sub, sub)
                    at = r * seq_dev + g * sub
                    att[pl.ds(start, sub), cols] = out[at : at + sub]
        product = lax.dot_general(
            wo_t[...], att[...], (((1,), (1,)), ((), ())), preferred_element_type=jnp.float32
        )
        keep[...] = product[:, : tokens // 2]
        send[...] = product[:, tokens // 2 :].astype(jnp.bfloat16)

    return body


def halve_body(keep, got, send, rest):
    half = rest.shape[1]
    rest[...] = keep[:, :half] + got[:, :half].astype(jnp.float32)
    send[...] = (keep[:, half:] + got[:, half:].astype(jnp.float32)).astype(jnp.bfloat16)


def carry_body(rest, got, resid, gain, carried, out):
    columns = rest.shape[0]
    total = rest[...] + got[...].astype(jnp.float32) + resid[...].astype(jnp.float32)
    carried[...] = total
    squares = jnp.sum(total * total, axis=0, keepdims=True)
    high = squares.astype(jnp.bfloat16)
    low = (squares - high.astype(jnp.float32)).astype(jnp.bfloat16)
    pick = lax.broadcasted_iota(jnp.int32, (16, total.shape[1]), 0)
    both = jnp.where(pick == 0, high.astype(jnp.float32), jnp.where(pick == 1, low.astype(jnp.float32), 0.0))
    out[pl.ds(0, columns), :] = (total * gain[...]).astype(jnp.bfloat16)
    out[pl.ds(columns, 16), :] = both.astype(jnp.bfloat16)


def gate_body(offsets, columns, units, tile, first, last):
    n = len(offsets)

    def body(place, *refs):
        pairs, weights, refs = list(zip(refs[:n], refs[n : 2 * n])), refs[2 * n], refs[2 * n + 1 :]
        sums, refs = (None, refs) if first else (refs[:3], refs[3:])
        spots = [pl.ds(pl.multiple_of((place[0] ^ r) * columns, 128), columns) for r in offsets]

        def both(rows):
            return [jnp.concatenate([own[rows, :], other[rows, :]], axis=1) for own, other in pairs]

        squares = sum(jnp.sum(b.astype(jnp.float32), axis=0, keepdims=True) for b in both(pl.ds(columns, 16)))
        if not first:
            squares = squares + sums[2][pl.ds(0, 1), :]
        scale = lax.rsqrt(squares / D + EPS) if last else None
        x = jnp.concatenate(both(pl.ds(0, columns)), axis=0)
        for start in range(0, units, tile):
            rows = pl.ds(start, tile)
            products = []
            for j in range(2):
                weight = jnp.concatenate([weights[pl.ds(j * units + start, tile), at] for at in spots], axis=1)
                part = jnp.dot(weight, x, preferred_element_type=jnp.float32)
                products.append(part if first else part + sums[j][rows, :])
            if last:
                gate, up = products[0] * scale, products[1] * scale
                refs[2][rows, :] = gate / (1.0 + jnp.exp(-gate)) * up
            else:
                refs[0][rows, :], refs[1][rows, :] = products
        if last:
            tokens = x.shape[1] // 2
            refs[0][...] = refs[2][:, :tokens].T.astype(jnp.bfloat16)
            refs[1][...] = refs[2][:, tokens:].T.astype(jnp.bfloat16)
        else:
            refs[2][...] = jnp.broadcast_to(squares, refs[2].shape)

    return body


def down_body(offsets, columns):
    def body(place, own, other, weights, *outs):
        units = own.shape[1]
        for r, out in zip(offsets, outs):
            at = pl.ds(pl.multiple_of((place[0] ^ r) * columns, 128), columns)
            total = jnp.dot(own[...], weights[pl.ds(0, units), at], preferred_element_type=jnp.float32)
            total = total + jnp.dot(other[...], weights[pl.ds(units, units), at], preferred_element_type=jnp.float32)
            out[...] = total.astype(out.dtype)

    return body


def turn_body(x, out):
    out[...] = x[...].T


def add_body(mine, got, out):
    out[...] = (mine[...].astype(jnp.float32) + got[...].astype(jnp.float32)).astype(out.dtype)


def finish_body(carried, mine, *refs):
    total = mine[...]
    for got in refs[:-1]:
        total = total + got[...].astype(jnp.float32)
    refs[-1][...] = (carried[...] + total.T).astype(jnp.bfloat16)


def exchanged(queries, keys, values, block_order, wo, resid, gain, w_gate, w_up, w_down):
    f32, bf16 = jnp.float32, jnp.bfloat16
    seq_dev, heads_features = queries.shape
    n_seq, reps = lax.axis_size("seq"), lax.axis_size("rep")
    groups = lax.axis_size("section") * reps
    tokens = n_seq * seq_dev
    group_tokens = tokens // groups
    columns = wo.shape[1]
    units = w_gate.shape[0]
    place = jnp.stack([lax.axis_index(a).astype(jnp.int32) for a in ("seq", "section", "rep")])
    place = jnp.concatenate([place, block_order])

    share = units // reps
    blocks = gather(stack([queries, keys, values]), n_seq)
    mine, theirs = (lambda p: p[2] * share), (lambda p: (1 - p[2]) * share)
    w_gate_up = fetch(place, [w_gate, w_up], share, (mine, mine))
    w_down = fetch(place, [w_down, w_down], share, (mine, theirs))
    wo_t = call(turn_body, struct(wo.shape[::-1], bf16), (wo,), limit=4)
    send, keep = call(
        attend_body(n_seq, seq_dev, heads_features // HEAD_DIM, groups, reps),
        (struct((columns, tokens // 2), bf16), struct((columns, tokens // 2), f32)),
        (place, *blocks, wo_t),
        scalars=1,
        scratch=[pltpu.VMEM((tokens, heads_features), bf16)],
        limit=8,
    )
    got = lax.ppermute(send, "rep", [(0, 1), (1, 0)])
    send, rest = call(
        halve_body, (struct((columns, group_tokens), bf16), struct((columns, group_tokens), f32)), (keep, got), limit=3
    )
    got = lax.ppermute(send, "section", [(0, 1), (1, 0)])
    gain_wide = jnp.broadcast_to(gain.astype(f32)[:, None], (columns, group_tokens))
    carried, x = call(
        carry_body,
        (struct((columns, group_tokens), f32), struct((columns + 16, group_tokens), bf16)),
        (rest, got, resid.reshape(columns, group_tokens), gain_wide),
        limit=3,
    )
    xs = gather(x, n_seq)

    def over_rep(x):
        return lax.ppermute(x, "rep", [(0, 1), (1, 0)])

    others = [over_rep(b) for b in xs]
    acc, tile = (), max(t for t in range(16, 601, 16) if share % t == 0)
    for i, offsets in enumerate(SHARES):
        first, last, n = i == 0, i == len(SHARES) - 1, len(offsets)
        if last:
            outs = (struct((group_tokens, share), bf16),) * 2
        else:
            outs = (struct((share, 2 * group_tokens), f32),) * 2 + (struct((8, 2 * group_tokens), f32),)
        acc = call(
            gate_body(offsets, columns, share, tile, first, last),
            outs,
            (place, *(xs[r] for r in offsets), *(others[r] for r in offsets), w_gate_up, *acc),
            scalars=1,
            scratch=[pltpu.VMEM((share, 2 * group_tokens), f32)] if last else [],
            limit=6,
            aliases={} if first or last else {1 + 2 * n + 1 + j: j for j in range(3)},
        )
    hidden = (acc[0], over_rep(acc[1]))

    def down(*offsets_types):
        return call(
            down_body([r for r, _ in offsets_types], columns),
            tuple(struct((group_tokens, columns), t) for _, t in offsets_types),
            (place, *hidden, w_down),
            scalars=1,
            limit=3,
        )

    def plus(mine, got):
        return call(add_body, struct((group_tokens, columns), bf16), (mine, got), limit=3)

    own, far = {}, {}
    far[6], = down((7, bf16))
    own[6], far[4] = down((6, f32), (5, bf16))
    own[4], far[2] = down((4, f32), (3, bf16))
    own[2], far[0], own[0] = down((2, f32), (1, bf16), (0, f32))
    got = {r: swap(far[r], 1, n_seq) for r in (6, 4, 2, 0)}
    sums = {6: plus(own[6], got[6])}
    onward = swap(sums[6], 2, n_seq)
    sums[2] = plus(own[2], got[2])
    sums[4] = plus(plus(own[4], got[4]), onward)
    parts = [got[0], swap(sums[2], 2, n_seq), swap(sums[4], 4, n_seq)]
    out = call(finish_body, struct((columns, group_tokens), bf16), (carried, own[0], *parts), limit=3)
    return out.reshape(resid.shape)


def on_device(queries, keys, values, block_order, wo, resid, gain, w_gate, w_up, w_down):
    groups = lax.axis_size("section") * lax.axis_size("rep")
    n_seq = lax.axis_size("seq")
    fits = (
        n_seq == SEQ
        and groups == 4
        and lax.axis_size("rep") == 2
        and wo.shape[1] % 128 == 0
        and (queries.shape[0] // groups) % 16 == 0
        and w_gate.shape[0] % 32 == 0
        and (queries.shape[0] * n_seq // groups) % 128 == 0
    )
    form = exchanged if fits else gathered
    return form(queries, keys, values, block_order, wo, resid, gain, w_gate, w_up, w_down)


def solution(mesh):
    return jax.shard_map(
        on_device,
        mesh=mesh,
        in_specs=(
            P("seq", ("section", "rep")),
            P("seq", ("section", "rep")),
            P("seq", ("section", "rep")),
            P(),
            P(("section", "rep"), "seq"),
            P(("section", "rep"), "seq", None),
            P("seq"),
            P("seq", None),
            P("seq", None),
            P("seq", None),
        ),
        out_specs=P(("section", "rep"), "seq", None),
        check_vma=False,
    )
```

```python
import jax
import jax.numpy as jnp
from jax import lax
from jax.experimental import pallas as pl
from jax.experimental.pallas import tpu as pltpu
from jax.sharding import PartitionSpec as P


D = 5120
HEAD_DIM = 128
EPS = 1e-05
LOG2E = 1.4426950408889634
MIB = 1 << 20
SEQ = 8
SHARES = ((0, 1), (2, 4), (5, 6), (3, 7))
VMEM = pl.BlockSpec(memory_space=pltpu.VMEM)
HBM = pl.BlockSpec(memory_space=pltpu.MemorySpace.HBM)
SMEM = pl.BlockSpec(memory_space=pltpu.SMEM)


def key_positions(order, start, count, block_rows):
    row_ids = start + jnp.arange(count, dtype=jnp.int32)
    owners = row_ids // block_rows
    match = owners[:, None] == jnp.arange(order.shape[0], dtype=jnp.int32)[None, :]
    first = jnp.sum(jnp.where(match, order[None, :], 0), axis=1)
    return first * block_rows + row_ids % block_rows


def gathered(queries, keys, values, block_order, wo, resid, gain, w_gate, w_up, w_down):
    seq_dev = queries.shape[0]
    heads_dev = queries.shape[1] // HEAD_DIM
    groups = lax.axis_size("section") * lax.axis_size("rep")
    n_seq = lax.axis_size("seq")
    sub_rows = seq_dev // groups
    block_rows = seq_dev // 2
    query_start = lax.axis_index("seq") * seq_dev
    query_pos = key_positions(block_order, query_start, seq_dev, block_rows)
    query_heads = queries.reshape(seq_dev, heads_dev, HEAD_DIM)
    scale = HEAD_DIM ** (-0.5)
    running_max = jnp.full((seq_dev, heads_dev), -1e30, jnp.float32)
    key_piece = lax.all_gather(keys, "seq", axis=0, tiled=True)
    value_piece = lax.all_gather(values, "seq", axis=0, tiled=True)
    count = key_piece.shape[0]
    key_pos = key_positions(block_order, jnp.int32(0), count, block_rows)
    scores = (
        jnp.einsum(
            "qhd,khd->qhk",
            query_heads,
            key_piece.reshape(count, heads_dev, HEAD_DIM),
            preferred_element_type=jnp.float32,
        )
        * scale
    )
    visible = (key_pos[None, :] <= query_pos[:, None])[:, None, :]
    new_max = jnp.maximum(running_max, jnp.max(jnp.where(visible, scores, -1e30), axis=-1))
    probs = jnp.where(visible, jnp.exp(scores - new_max[..., None]), 0.0)
    total = jnp.sum(probs, axis=-1)
    weighted = jnp.einsum(
        "qhk,khd->qhd",
        probs.astype(jnp.bfloat16),
        value_piece.reshape(count, heads_dev, HEAD_DIM),
        preferred_element_type=jnp.float32,
    )
    running_max, total, weighted = (new_max, total, weighted)
    attended = (
        (weighted / total[..., None]).astype(jnp.bfloat16).reshape(seq_dev, heads_dev * HEAD_DIM)
    )
    columns = wo.shape[1]
    token_count = n_seq * sub_rows
    parts = attended.reshape(groups, sub_rows, heads_dev * HEAD_DIM)
    group_rows = lax.all_to_all(parts, ("section", "rep"), split_axis=0, concat_axis=2, tiled=True)
    wo_columns = lax.all_gather(wo, ("section", "rep"), axis=0, tiled=True)
    piece = lax.all_gather(group_rows, "seq", axis=0, tiled=True)
    flat = piece.reshape(piece.shape[0] * piece.shape[1], piece.shape[2])
    product = jnp.dot(flat, wo_columns, preferred_element_type=jnp.float32)
    projected = product.reshape(piece.shape[0], piece.shape[1], columns)
    projected_cols = projected.reshape(token_count, columns).T
    carried = resid.reshape(columns, token_count).astype(jnp.float32) + projected_cols
    squares = lax.psum(jnp.sum(carried * carried, axis=0), "seq")
    normed = (
        carried * lax.rsqrt(squares / D + 1e-05)[None, :] * gain.astype(jnp.float32)[:, None]
    ).astype(jnp.bfloat16)
    piece = lax.all_gather(normed, "seq", axis=0, tiled=True)
    gate_sum = jnp.dot(w_gate, piece, preferred_element_type=jnp.float32)
    up_sum = jnp.dot(w_up, piece, preferred_element_type=jnp.float32)
    hidden = (jax.nn.silu(gate_sum) * up_sum).astype(jnp.bfloat16)
    term = lax.dot_general(
        w_down, hidden, (((0,), (0,)), ((), ())), preferred_element_type=jnp.float32
    )
    down = lax.psum_scatter(term, "seq", scatter_dimension=0, tiled=True)
    return (carried + down).astype(jnp.bfloat16).reshape(resid.shape)


def call(body, outs, args, scalars=0, scratch=(), limit=7, aliases=None, in_place=()):
    spaces = [SMEM] * scalars + [VMEM] * (len(args) - scalars)
    for i in in_place:
        spaces[i] = HBM
    return pl.pallas_call(
        body,
        out_shape=outs,
        in_specs=spaces,
        out_specs=jax.tree.map(lambda _: VMEM, outs),
        scratch_shapes=list(scratch),
        input_output_aliases=aliases or {},
        compiler_params=pltpu.CompilerParams(vmem_limit_bytes=limit * MIB),
        cost_estimate=pl.CostEstimate(flops=0, bytes_accessed=0, transcendentals=0),
    )(*args)


def struct(shape, dtype):
    return jax.ShapeDtypeStruct(shape, dtype)


def swap(x, offset, n_seq):
    return lax.ppermute(x, "seq", [(i, i ^ offset) for i in range(n_seq)])


def gather(x, n_seq):
    got = {r: swap(x, r, n_seq) for r in (4, 1, 2)}
    for r, source, offset in ((5, 4, 1), (6, 4, 2), (3, 2, 1), (7, 5, 2)):
        got[r] = swap(got[source], offset, n_seq)
    return [x] + [got[r] for r in range(1, n_seq)]


def in_hbm(x):
    return pltpu.with_memory_space_constraint(x, pltpu.MemorySpace.HBM)


def fetch(place, arrays, rows, bases):
    n, width = len(arrays), arrays[0].shape[1]

    def body(place, *refs):
        ins, out, sems = refs[:n], refs[n], refs[n + 1]
        copies = []
        for i, (source, base) in enumerate(zip(ins, bases)):
            start = pl.multiple_of(base(place), 16)
            copies.append(pltpu.make_async_copy(source.at[pl.ds(start, rows)], out.at[pl.ds(i * rows, rows)], sems.at[i]))
        for c in copies:
            c.start()
        for c in copies:
            c.wait()

    return pl.pallas_call(
        body,
        out_shape=pltpu.VMEM((n * rows, width), arrays[0].dtype),
        in_specs=[SMEM] + [HBM] * n,
        out_specs=VMEM,
        scratch_shapes=[pltpu.SemaphoreType.DMA((n,))],
        compiler_params=pltpu.CompilerParams(vmem_limit_bytes=MIB),
    )(place, *(in_hbm(a) for a in arrays))


def stack(arrays):
    rows, width = arrays[0].shape

    def body(*refs):
        ins, out, sems = refs[:-2], refs[-2], refs[-1]
        copies = [pltpu.make_async_copy(ref, out.at[pl.ds(i * rows, rows)], sems.at[i]) for i, ref in enumerate(ins)]
        for c in copies:
            c.start()
        for c in copies:
            c.wait()

    n = len(arrays)
    return pl.pallas_call(
        body,
        name="stack",
        out_shape=pltpu.VMEM((n * rows, width), arrays[0].dtype),
        in_specs=[HBM] * n,
        out_specs=VMEM,
        scratch_shapes=[pltpu.SemaphoreType.DMA((n,))],
        compiler_params=pltpu.CompilerParams(vmem_limit_bytes=MIB),
    )(*(in_hbm(a) for a in arrays))


def attend_body(n_seq, seq_dev, heads_dev, groups, reps):
    sub = seq_dev // groups
    half = seq_dev // 2
    tokens = n_seq * seq_dev
    per_group = n_seq * sub

    def body(place, *refs):
        blocks, wo_t, send, keep, att = refs[:n_seq], *refs[n_seq:]
        me, section, rep = place[0], place[1], place[2]
        lane = lax.broadcasted_iota(jnp.int32, (1, tokens), 1)
        row = lax.broadcasted_iota(jnp.int32, (seq_dev, 1), 0)
        key_pos = jnp.zeros((1, tokens), jnp.int32)
        query_pos = []
        for r in range(n_seq):
            source = me ^ r
            low, high = place[3 + 2 * source] * half, place[4 + 2 * source] * half
            key_pos = jnp.where(lane >= r * seq_dev, low + lane - r * seq_dev, key_pos)
            key_pos = jnp.where(lane >= r * seq_dev + half, high + lane - r * seq_dev - half, key_pos)
            query_pos.append(jnp.where(row < half, low + row, high + row - half))
        query_pos = jnp.concatenate(query_pos, axis=0)
        for h in range(heads_dev):
            cols = pl.ds(h * HEAD_DIM, HEAD_DIM)
            q, k, v = (
                jnp.concatenate([b[pl.ds(i * seq_dev, seq_dev), cols] for b in blocks], axis=0)
                for i in range(3)
            )
            scores = lax.dot_general(q, k, (((1,), (1,)), ((), ())), preferred_element_type=jnp.float32)
            scores = jnp.where(key_pos <= query_pos, scores, -1e30)
            top = jnp.max(scores, axis=-1, keepdims=True)
            probs = jnp.exp2((scores - top) * (HEAD_DIM**-0.5 * LOG2E))
            total = jnp.sum(probs, axis=-1, keepdims=True)
            out = jnp.dot(probs.astype(jnp.bfloat16), v, preferred_element_type=jnp.float32)
            out = (out / total).astype(jnp.bfloat16)
            for r in range(n_seq):
                source = me ^ r
                for g in range(groups):
                    slot = ((g % reps) ^ rep) * (groups // reps) + ((g // reps) ^ section)
                    start = pl.multiple_of(slot * per_group + source * sub, sub)
                    at = r * seq_dev + g * sub
                    att[pl.ds(start, sub), cols] = out[at : at + sub]
        product = lax.dot_general(
            wo_t[...], att[...], (((1,), (1,)), ((), ())), preferred_element_type=jnp.float32
        )
        keep[...] = product[:, : tokens // 2]
        send[...] = product[:, tokens // 2 :].astype(jnp.bfloat16)

    return body


def halve_body(keep, got, send, rest):
    half = rest.shape[1]
    rest[...] = keep[:, :half] + got[:, :half].astype(jnp.float32)
    send[...] = (keep[:, half:] + got[:, half:].astype(jnp.float32)).astype(jnp.bfloat16)


def carry_body(rest, got, resid, gain, carried, out):
    columns = rest.shape[0]
    total = rest[...] + got[...].astype(jnp.float32) + resid[...].astype(jnp.float32)
    carried[...] = total
    squares = jnp.sum(total * total, axis=0, keepdims=True)
    high = squares.astype(jnp.bfloat16)
    low = (squares - high.astype(jnp.float32)).astype(jnp.bfloat16)
    pick = lax.broadcasted_iota(jnp.int32, (16, total.shape[1]), 0)
    both = jnp.where(pick == 0, high.astype(jnp.float32), jnp.where(pick == 1, low.astype(jnp.float32), 0.0))
    out[pl.ds(0, columns), :] = (total * gain[...]).astype(jnp.bfloat16)
    out[pl.ds(columns, 16), :] = both.astype(jnp.bfloat16)


def gate_body(offsets, columns, units, tile, first, last):
    n = len(offsets)

    def body(place, *refs):
        pairs, weights, refs = list(zip(refs[:n], refs[n : 2 * n])), refs[2 * n], refs[2 * n + 1 :]
        sums, refs = (None, refs) if first else (refs[:3], refs[3:])
        spots = [pl.ds(pl.multiple_of((place[0] ^ r) * columns, 128), columns) for r in offsets]

        def both(rows):
            return [jnp.concatenate([own[rows, :], other[rows, :]], axis=1) for own, other in pairs]

        squares = sum(jnp.sum(b.astype(jnp.float32), axis=0, keepdims=True) for b in both(pl.ds(columns, 16)))
        if not first:
            squares = squares + sums[2][pl.ds(0, 1), :]
        scale = lax.rsqrt(squares / D + EPS) if last else None
        x = jnp.concatenate(both(pl.ds(0, columns)), axis=0)
        for start in range(0, units, tile):
            rows = pl.ds(start, tile)
            products = []
            for j in range(2):
                weight = jnp.concatenate([weights[pl.ds(j * units + start, tile), at] for at in spots], axis=1)
                part = jnp.dot(weight, x, preferred_element_type=jnp.float32)
                products.append(part if first else part + sums[j][rows, :])
            if last:
                gate, up = products[0] * scale, products[1] * scale
                refs[2][rows, :] = gate / (1.0 + jnp.exp(-gate)) * up
            else:
                refs[0][rows, :], refs[1][rows, :] = products
        if last:
            tokens = x.shape[1] // 2
            refs[0][...] = refs[2][:, :tokens].T.astype(jnp.bfloat16)
            refs[1][...] = refs[2][:, tokens:].T.astype(jnp.bfloat16)
        else:
            refs[2][...] = jnp.broadcast_to(squares, refs[2].shape)

    return body


def down_body(offsets, columns):
    def body(place, own, other, w_own, w_other, *outs):
        for r, out in zip(offsets, outs):
            at = pl.ds(pl.multiple_of((place[0] ^ r) * columns, 128), columns)
            total = jnp.dot(own[...], w_own[:, at], preferred_element_type=jnp.float32)
            total = total + jnp.dot(other[...], w_other[:, at], preferred_element_type=jnp.float32)
            out[...] = total.astype(out.dtype)

    return body


def turn_body(x, out):
    out[...] = x[...].T


def add_body(mine, got, out):
    out[...] = (mine[...].astype(jnp.float32) + got[...].astype(jnp.float32)).astype(out.dtype)


def finish_body(carried, mine, *refs):
    total = mine[...]
    for got in refs[:-1]:
        total = total + got[...].astype(jnp.float32)
    refs[-1][...] = (carried[...] + total.T).astype(jnp.bfloat16)


def exchanged(queries, keys, values, block_order, wo, resid, gain, w_gate, w_up, w_down):
    f32, bf16 = jnp.float32, jnp.bfloat16
    seq_dev, heads_features = queries.shape
    n_seq, reps = lax.axis_size("seq"), lax.axis_size("rep")
    groups = lax.axis_size("section") * reps
    tokens = n_seq * seq_dev
    group_tokens = tokens // groups
    columns = wo.shape[1]
    units = w_gate.shape[0]
    place = jnp.stack([lax.axis_index(a).astype(jnp.int32) for a in ("seq", "section", "rep")])
    place = jnp.concatenate([place, block_order])

    share = units // reps
    blocks = gather(stack([queries, keys, values]), n_seq)
    mine, theirs = (lambda p: p[2] * share), (lambda p: (1 - p[2]) * share)
    w_gate_up = fetch(place, [w_gate, w_up], share, (mine, mine))
    w_down = [fetch(place, [w_down], share, (base,)) for base in (mine, theirs)]
    wo_t = call(turn_body, struct(wo.shape[::-1], bf16), (wo,), limit=4)
    send, keep = call(
        attend_body(n_seq, seq_dev, heads_features // HEAD_DIM, groups, reps),
        (struct((columns, tokens // 2), bf16), struct((columns, tokens // 2), f32)),
        (place, *blocks, wo_t),
        scalars=1,
        scratch=[pltpu.VMEM((tokens, heads_features), bf16)],
        limit=8,
    )
    got = lax.ppermute(send, "rep", [(0, 1), (1, 0)])
    send, rest = call(
        halve_body, (struct((columns, group_tokens), bf16), struct((columns, group_tokens), f32)), (keep, got), limit=3
    )
    got = lax.ppermute(send, "section", [(0, 1), (1, 0)])
    gain_wide = jnp.broadcast_to(gain.astype(f32)[:, None], (columns, group_tokens))
    carried, x = call(
        carry_body,
        (struct((columns, group_tokens), f32), struct((columns + 16, group_tokens), bf16)),
        (rest, got, resid.reshape(columns, group_tokens), gain_wide),
        limit=3,
    )
    xs = gather(x, n_seq)

    def over_rep(x):
        return lax.ppermute(x, "rep", [(0, 1), (1, 0)])

    others = [over_rep(b) for b in xs]
    acc, tile = (), max(t for t in range(16, 601, 16) if share % t == 0)
    for i, offsets in enumerate(SHARES):
        first, last, n = i == 0, i == len(SHARES) - 1, len(offsets)
        if last:
            outs = (struct((group_tokens, share), bf16),) * 2
        else:
            outs = (struct((share, 2 * group_tokens), f32),) * 2 + (struct((8, 2 * group_tokens), f32),)
        acc = call(
            gate_body(offsets, columns, share, tile, first, last),
            outs,
            (place, *(xs[r] for r in offsets), *(others[r] for r in offsets), w_gate_up, *acc),
            scalars=1,
            scratch=[pltpu.VMEM((share, 2 * group_tokens), f32)] if last else [],
            limit=6,
            aliases={} if first or last else {1 + 2 * n + 1 + j: j for j in range(3)},
        )
    hidden = (acc[0], over_rep(acc[1]))

    def down(*offsets_types):
        return call(
            down_body([r for r, _ in offsets_types], columns),
            tuple(struct((group_tokens, columns), t) for _, t in offsets_types),
            (place, *hidden, *w_down),
            scalars=1,
            limit=3,
        )

    def plus(mine, got):
        return call(add_body, struct((group_tokens, columns), bf16), (mine, got), limit=3)

    own, far = {}, {}
    far[6], = down((7, bf16))
    own[6], far[4] = down((6, f32), (5, bf16))
    own[4], far[2] = down((4, f32), (3, bf16))
    own[2], far[0], own[0] = down((2, f32), (1, bf16), (0, f32))
    got = {r: swap(far[r], 1, n_seq) for r in (6, 4, 2, 0)}
    sums = {6: plus(own[6], got[6])}
    onward = swap(sums[6], 2, n_seq)
    sums[2] = plus(own[2], got[2])
    sums[4] = plus(plus(own[4], got[4]), onward)
    parts = [got[0], swap(sums[2], 2, n_seq), swap(sums[4], 4, n_seq)]
    out = call(finish_body, struct((columns, group_tokens), bf16), (carried, own[0], *parts), limit=3)
    return out.reshape(resid.shape)


def on_device(queries, keys, values, block_order, wo, resid, gain, w_gate, w_up, w_down):
    groups = lax.axis_size("section") * lax.axis_size("rep")
    n_seq = lax.axis_size("seq")
    fits = (
        n_seq == SEQ
        and groups == 4
        and lax.axis_size("rep") == 2
        and wo.shape[1] % 128 == 0
        and (queries.shape[0] // groups) % 16 == 0
        and w_gate.shape[0] % 32 == 0
        and (queries.shape[0] * n_seq // groups) % 128 == 0
    )
    form = exchanged if fits else gathered
    return form(queries, keys, values, block_order, wo, resid, gain, w_gate, w_up, w_down)


def solution(mesh):
    return jax.shard_map(
        on_device,
        mesh=mesh,
        in_specs=(
            P("seq", ("section", "rep")),
            P("seq", ("section", "rep")),
            P("seq", ("section", "rep")),
            P(),
            P(("section", "rep"), "seq"),
            P(("section", "rep"), "seq", None),
            P("seq"),
            P("seq", None),
            P("seq", None),
            P("seq", None),
        ),
        out_specs=P(("section", "rep"), "seq", None),
        check_vma=False,
    )
```

```python
import jax
import jax.numpy as jnp
from jax import lax
from jax.experimental import pallas as pl
from jax.experimental.pallas import tpu as pltpu
from jax.sharding import PartitionSpec as P


D = 5120
HEAD_DIM = 128
EPS = 1e-05
LOG2E = 1.4426950408889634
MIB = 1 << 20
SEQ = 8
PRE = (7, 6, 3)
SHARES = ((0, 1), (2, 4), (5, 6), (3, 7))
VMEM = pl.BlockSpec(memory_space=pltpu.VMEM)
HBM = pl.BlockSpec(memory_space=pltpu.MemorySpace.HBM)
SMEM = pl.BlockSpec(memory_space=pltpu.SMEM)


def key_positions(order, start, count, block_rows):
    row_ids = start + jnp.arange(count, dtype=jnp.int32)
    owners = row_ids // block_rows
    match = owners[:, None] == jnp.arange(order.shape[0], dtype=jnp.int32)[None, :]
    first = jnp.sum(jnp.where(match, order[None, :], 0), axis=1)
    return first * block_rows + row_ids % block_rows


def gathered(queries, keys, values, block_order, wo, resid, gain, w_gate, w_up, w_down):
    seq_dev = queries.shape[0]
    heads_dev = queries.shape[1] // HEAD_DIM
    groups = lax.axis_size("section") * lax.axis_size("rep")
    n_seq = lax.axis_size("seq")
    sub_rows = seq_dev // groups
    block_rows = seq_dev // 2
    query_start = lax.axis_index("seq") * seq_dev
    query_pos = key_positions(block_order, query_start, seq_dev, block_rows)
    query_heads = queries.reshape(seq_dev, heads_dev, HEAD_DIM)
    scale = HEAD_DIM ** (-0.5)
    running_max = jnp.full((seq_dev, heads_dev), -1e30, jnp.float32)
    key_piece = lax.all_gather(keys, "seq", axis=0, tiled=True)
    value_piece = lax.all_gather(values, "seq", axis=0, tiled=True)
    count = key_piece.shape[0]
    key_pos = key_positions(block_order, jnp.int32(0), count, block_rows)
    scores = (
        jnp.einsum(
            "qhd,khd->qhk",
            query_heads,
            key_piece.reshape(count, heads_dev, HEAD_DIM),
            preferred_element_type=jnp.float32,
        )
        * scale
    )
    visible = (key_pos[None, :] <= query_pos[:, None])[:, None, :]
    new_max = jnp.maximum(running_max, jnp.max(jnp.where(visible, scores, -1e30), axis=-1))
    probs = jnp.where(visible, jnp.exp(scores - new_max[..., None]), 0.0)
    total = jnp.sum(probs, axis=-1)
    weighted = jnp.einsum(
        "qhk,khd->qhd",
        probs.astype(jnp.bfloat16),
        value_piece.reshape(count, heads_dev, HEAD_DIM),
        preferred_element_type=jnp.float32,
    )
    running_max, total, weighted = (new_max, total, weighted)
    attended = (
        (weighted / total[..., None]).astype(jnp.bfloat16).reshape(seq_dev, heads_dev * HEAD_DIM)
    )
    columns = wo.shape[1]
    token_count = n_seq * sub_rows
    parts = attended.reshape(groups, sub_rows, heads_dev * HEAD_DIM)
    group_rows = lax.all_to_all(parts, ("section", "rep"), split_axis=0, concat_axis=2, tiled=True)
    wo_columns = lax.all_gather(wo, ("section", "rep"), axis=0, tiled=True)
    piece = lax.all_gather(group_rows, "seq", axis=0, tiled=True)
    flat = piece.reshape(piece.shape[0] * piece.shape[1], piece.shape[2])
    product = jnp.dot(flat, wo_columns, preferred_element_type=jnp.float32)
    projected = product.reshape(piece.shape[0], piece.shape[1], columns)
    projected_cols = projected.reshape(token_count, columns).T
    carried = resid.reshape(columns, token_count).astype(jnp.float32) + projected_cols
    squares = lax.psum(jnp.sum(carried * carried, axis=0), "seq")
    normed = (
        carried * lax.rsqrt(squares / D + 1e-05)[None, :] * gain.astype(jnp.float32)[:, None]
    ).astype(jnp.bfloat16)
    piece = lax.all_gather(normed, "seq", axis=0, tiled=True)
    gate_sum = jnp.dot(w_gate, piece, preferred_element_type=jnp.float32)
    up_sum = jnp.dot(w_up, piece, preferred_element_type=jnp.float32)
    hidden = (jax.nn.silu(gate_sum) * up_sum).astype(jnp.bfloat16)
    term = lax.dot_general(
        w_down, hidden, (((0,), (0,)), ((), ())), preferred_element_type=jnp.float32
    )
    down = lax.psum_scatter(term, "seq", scatter_dimension=0, tiled=True)
    return (carried + down).astype(jnp.bfloat16).reshape(resid.shape)


def call(body, outs, args, scalars=0, scratch=(), limit=7, aliases=None, in_place=()):
    spaces = [SMEM] * scalars + [VMEM] * (len(args) - scalars)
    for i in in_place:
        spaces[i] = HBM
    return pl.pallas_call(
        body,
        out_shape=outs,
        in_specs=spaces,
        out_specs=jax.tree.map(lambda _: VMEM, outs),
        scratch_shapes=list(scratch),
        input_output_aliases=aliases or {},
        compiler_params=pltpu.CompilerParams(vmem_limit_bytes=limit * MIB),
        cost_estimate=pl.CostEstimate(flops=0, bytes_accessed=0, transcendentals=0),
    )(*args)


def struct(shape, dtype):
    return jax.ShapeDtypeStruct(shape, dtype)


def swap(x, offset, n_seq):
    return lax.ppermute(x, "seq", [(i, i ^ offset) for i in range(n_seq)])


def gather(x, n_seq):
    got = {r: swap(x, r, n_seq) for r in (4, 1, 2)}
    for r, source, offset in ((5, 4, 1), (6, 4, 2), (3, 2, 1), (7, 5, 2)):
        got[r] = swap(got[source], offset, n_seq)
    return [x] + [got[r] for r in range(1, n_seq)]


def in_hbm(x):
    return pltpu.with_memory_space_constraint(x, pltpu.MemorySpace.HBM)


def fetch(place, arrays, rows, bases):
    n, width = len(arrays), arrays[0].shape[1]

    def body(place, *refs):
        ins, out, sems = refs[:n], refs[n], refs[n + 1]
        copies = []
        for i, (source, base) in enumerate(zip(ins, bases)):
            start = pl.multiple_of(base(place), 16)
            copies.append(pltpu.make_async_copy(source.at[pl.ds(start, rows)], out.at[pl.ds(i * rows, rows)], sems.at[i]))
        for c in copies:
            c.start()
        for c in copies:
            c.wait()

    return pl.pallas_call(
        body,
        out_shape=pltpu.VMEM((n * rows, width), arrays[0].dtype),
        in_specs=[SMEM] + [HBM] * n,
        out_specs=VMEM,
        scratch_shapes=[pltpu.SemaphoreType.DMA((n,))],
        compiler_params=pltpu.CompilerParams(vmem_limit_bytes=MIB),
    )(place, *(in_hbm(a) for a in arrays))


def stack(arrays):
    rows, width = arrays[0].shape

    def body(*refs):
        ins, out, sems = refs[:-2], refs[-2], refs[-1]
        copies = [pltpu.make_async_copy(ref, out.at[pl.ds(i * rows, rows)], sems.at[i]) for i, ref in enumerate(ins)]
        for c in copies:
            c.start()
        for c in copies:
            c.wait()

    n = len(arrays)
    return pl.pallas_call(
        body,
        name="stack",
        out_shape=pltpu.VMEM((n * rows, width), arrays[0].dtype),
        in_specs=[HBM] * n,
        out_specs=VMEM,
        scratch_shapes=[pltpu.SemaphoreType.DMA((n,))],
        compiler_params=pltpu.CompilerParams(vmem_limit_bytes=MIB),
    )(*(in_hbm(a) for a in arrays))


def attend_body(n_seq, seq_dev, heads_dev, groups, reps):
    sub = seq_dev // groups
    half = seq_dev // 2
    tokens = n_seq * seq_dev
    per_group = n_seq * sub

    def body(place, *refs):
        blocks, wo_t, send, keep, att = refs[:n_seq], *refs[n_seq:]
        me, section, rep = place[0], place[1], place[2]
        lane = lax.broadcasted_iota(jnp.int32, (1, tokens), 1)
        row = lax.broadcasted_iota(jnp.int32, (seq_dev, 1), 0)
        key_pos = jnp.zeros((1, tokens), jnp.int32)
        query_pos = []
        for r in range(n_seq):
            source = me ^ r
            low, high = place[3 + 2 * source] * half, place[4 + 2 * source] * half
            key_pos = jnp.where(lane >= r * seq_dev, low + lane - r * seq_dev, key_pos)
            key_pos = jnp.where(lane >= r * seq_dev + half, high + lane - r * seq_dev - half, key_pos)
            query_pos.append(jnp.where(row < half, low + row, high + row - half))
        query_pos = jnp.concatenate(query_pos, axis=0)
        for h in range(heads_dev):
            cols = pl.ds(h * HEAD_DIM, HEAD_DIM)
            q, k, v = (
                jnp.concatenate([b[pl.ds(i * seq_dev, seq_dev), cols] for b in blocks], axis=0)
                for i in range(3)
            )
            scores = lax.dot_general(q, k, (((1,), (1,)), ((), ())), preferred_element_type=jnp.float32)
            scores = jnp.where(key_pos <= query_pos, scores, -1e30)
            top = jnp.max(scores, axis=-1, keepdims=True)
            probs = jnp.exp2((scores - top) * (HEAD_DIM**-0.5 * LOG2E))
            total = jnp.sum(probs, axis=-1, keepdims=True)
            out = jnp.dot(probs.astype(jnp.bfloat16), v, preferred_element_type=jnp.float32)
            out = (out / total).astype(jnp.bfloat16)
            for r in range(n_seq):
                source = me ^ r
                for g in range(groups):
                    slot = ((g % reps) ^ rep) * (groups // reps) + ((g // reps) ^ section)
                    start = pl.multiple_of(slot * per_group + source * sub, sub)
                    at = r * seq_dev + g * sub
                    att[pl.ds(start, sub), cols] = out[at : at + sub]
        product = lax.dot_general(
            wo_t[...], att[...], (((1,), (1,)), ((), ())), preferred_element_type=jnp.float32
        )
        keep[...] = product[:, : tokens // 2]
        send[...] = product[:, tokens // 2 :].astype(jnp.bfloat16)

    return body


def halve_body(keep, got, send, rest):
    half = rest.shape[1]
    rest[...] = keep[:, :half] + got[:, :half].astype(jnp.float32)
    send[...] = (keep[:, half:] + got[:, half:].astype(jnp.float32)).astype(jnp.bfloat16)


def carry_body(rest, got, resid, gain, carried, out):
    columns = rest.shape[0]
    total = rest[...] + got[...].astype(jnp.float32) + resid[...].astype(jnp.float32)
    carried[...] = total
    squares = jnp.sum(total * total, axis=0, keepdims=True)
    high = squares.astype(jnp.bfloat16)
    low = (squares - high.astype(jnp.float32)).astype(jnp.bfloat16)
    pick = lax.broadcasted_iota(jnp.int32, (16, total.shape[1]), 0)
    both = jnp.where(pick == 0, high.astype(jnp.float32), jnp.where(pick == 1, low.astype(jnp.float32), 0.0))
    out[pl.ds(0, columns), :] = (total * gain[...]).astype(jnp.bfloat16)
    out[pl.ds(columns, 16), :] = both.astype(jnp.bfloat16)


def gate_body(offsets, columns, units, tile, first, last):
    n = len(offsets)

    def body(place, *refs):
        pairs, weights, refs = list(zip(refs[:n], refs[n : 2 * n])), refs[2 * n], refs[2 * n + 1 :]
        sums, refs = (None, refs) if first else (refs[:3], refs[3:])
        spots = [pl.ds(pl.multiple_of((place[0] ^ r) * columns, 128), columns) for r in offsets]

        def both(rows):
            return [jnp.concatenate([own[rows, :], other[rows, :]], axis=1) for own, other in pairs]

        squares = sum(jnp.sum(b.astype(jnp.float32), axis=0, keepdims=True) for b in both(pl.ds(columns, 16)))
        if not first:
            squares = squares + sums[2][pl.ds(0, 1), :]
        scale = lax.rsqrt(squares / D + EPS) if last else None
        x = jnp.concatenate(both(pl.ds(0, columns)), axis=0)
        for start in range(0, units, tile):
            rows = pl.ds(start, tile)
            products = []
            for j in range(2):
                weight = jnp.concatenate([weights[pl.ds(j * units + start, tile), at] for at in spots], axis=1)
                part = jnp.dot(weight, x, preferred_element_type=jnp.float32)
                products.append(part if first else part + sums[j][rows, :])
            if last:
                gate, up = products[0] * scale, products[1] * scale
                refs[2][rows, :] = gate / (1.0 + jnp.exp(-gate)) * up
            else:
                refs[0][rows, :], refs[1][rows, :] = products
        if last:
            tokens = x.shape[1] // 2
            refs[0][...] = refs[2][:, :tokens].T.astype(jnp.bfloat16)
            refs[1][...] = refs[2][:, tokens:].T.astype(jnp.bfloat16)
        else:
            refs[2][...] = jnp.broadcast_to(squares, refs[2].shape)

    return body


def down_body(offsets, columns, parts):
    def body(place, *refs):
        hidden, weights, refs = refs[:parts], refs[parts : 2 * parts], refs[2 * parts :]
        outs, given = refs[-len(offsets) :], refs[: -len(offsets)]
        for i, (r, out) in enumerate(zip(offsets, outs)):
            at = pl.ds(pl.multiple_of((place[0] ^ r) * columns, 128), columns)
            total = given[i][...] if given else None
            for units, weight in zip(hidden, weights):
                part = jnp.dot(units[...], weight[:, at], preferred_element_type=jnp.float32)
                total = part if total is None else total + part
            out[...] = total.astype(out.dtype)

    return body


def turn_body(x, gain, out, gain_wide):
    out[...] = x[...].T
    gain_wide[...] = jnp.broadcast_to(gain[...].astype(jnp.float32), gain_wide.shape[::-1]).T


def add_body(*refs):
    total = refs[0][...].astype(jnp.float32)
    for ref in refs[1:-1]:
        total = total + ref[...].astype(jnp.float32)
    refs[-1][...] = total.astype(refs[-1].dtype)


def finish_body(carried, mine, *refs):
    total = mine[...]
    for got in refs[:-1]:
        total = total + got[...].astype(jnp.float32)
    refs[-1][...] = (carried[...] + total.T).astype(jnp.bfloat16)


def exchanged(queries, keys, values, block_order, wo, resid, gain, w_gate, w_up, w_down):
    f32, bf16 = jnp.float32, jnp.bfloat16
    seq_dev, heads_features = queries.shape
    n_seq, reps = lax.axis_size("seq"), lax.axis_size("rep")
    groups = lax.axis_size("section") * reps
    tokens = n_seq * seq_dev
    group_tokens = tokens // groups
    columns = wo.shape[1]
    units = w_gate.shape[0]
    place = jnp.stack([lax.axis_index(a).astype(jnp.int32) for a in ("seq", "section", "rep")])
    place = jnp.concatenate([place, block_order])

    share = units // reps
    blocks = gather(stack([queries, keys, values]), n_seq)
    mine, theirs = (lambda p: p[2] * share), (lambda p: (1 - p[2]) * share)
    w_gate_up = fetch(place, [w_gate, w_up], share, (mine, mine))
    w_down = [fetch(place, [w_down], share, (base,)) for base in (mine, theirs)]
    wo_t, gain_wide = call(
        turn_body,
        (struct(wo.shape[::-1], bf16), struct((columns, group_tokens), f32)),
        (wo, gain.reshape(1, columns)),
        limit=4,
    )
    send, keep = call(
        attend_body(n_seq, seq_dev, heads_features // HEAD_DIM, groups, reps),
        (struct((columns, tokens // 2), bf16), struct((columns, tokens // 2), f32)),
        (place, *blocks, wo_t),
        scalars=1,
        scratch=[pltpu.VMEM((tokens, heads_features), bf16)],
        limit=8,
    )
    got = lax.ppermute(send, "rep", [(0, 1), (1, 0)])
    send, rest = call(
        halve_body, (struct((columns, group_tokens), bf16), struct((columns, group_tokens), f32)), (keep, got), limit=3
    )
    got = lax.ppermute(send, "section", [(0, 1), (1, 0)])
    carried, x = call(
        carry_body,
        (struct((columns, group_tokens), f32), struct((columns + 16, group_tokens), bf16)),
        (rest, got, resid.reshape(columns, group_tokens), gain_wide),
        limit=3,
    )
    xs = gather(x, n_seq)

    def over_rep(x):
        return lax.ppermute(x, "rep", [(0, 1), (1, 0)])

    others = [over_rep(b) for b in xs]
    acc, tile = (), max(t for t in range(16, 601, 16) if share % t == 0)
    for i, offsets in enumerate(SHARES):
        first, last, n = i == 0, i == len(SHARES) - 1, len(offsets)
        if last:
            outs = (struct((group_tokens, share), bf16),) * 2
        else:
            outs = (struct((share, 2 * group_tokens), f32),) * 2 + (struct((8, 2 * group_tokens), f32),)
        acc = call(
            gate_body(offsets, columns, share, tile, first, last),
            outs,
            (place, *(xs[r] for r in offsets), *(others[r] for r in offsets), w_gate_up, *acc),
            scalars=1,
            scratch=[pltpu.VMEM((share, 2 * group_tokens), f32)] if last else [],
            limit=6,
            aliases={} if first or last else {1 + 2 * n + 1 + j: j for j in range(3)},
        )
    hidden = (acc[0], over_rep(acc[1]))
    block = (group_tokens, columns)
    before = dict(
        zip(
            PRE,
            call(
                down_body(PRE, columns, 1),
                (struct(block, f32),) * len(PRE),
                (place, hidden[0], w_down[0]),
                scalars=1,
                limit=3,
            ),
        )
    )

    def down(*offsets_types):
        offsets = [r for r, _ in offsets_types]
        given = [before[r] for r in offsets if r in before]
        units = ((hidden[1], w_down[1]) if given else (*hidden, *w_down))
        return call(
            down_body(offsets, columns, len(units) // 2),
            tuple(struct(block, t) for _, t in offsets_types),
            (place, *units, *given),
            scalars=1,
            limit=3,
        )

    def plus(*terms):
        return call(add_body, struct(block, bf16), terms, limit=3)

    (p7,) = down((7, bf16))
    p6, p3 = down((6, bf16), (3, bf16))
    p5, p2 = down((5, f32), (2, f32))
    p4, p1, p0 = down((4, f32), (1, bf16), (0, f32))
    got7, got6, got3, got1 = (swap(p, offset, n_seq) for p, offset in ((p7, 2), (p6, 2), (p3, 1), (p1, 1)))
    got5 = swap(plus(p5, got7), 1, n_seq)
    got2 = swap(plus(p2, got3), 2, n_seq)
    got4 = swap(plus(p4, got6, got5), 4, n_seq)
    parts = (got1, got2, got4)
    out = call(finish_body, struct((columns, group_tokens), bf16), (carried, p0, *parts), limit=3)
    return out.reshape(resid.shape)


def on_device(queries, keys, values, block_order, wo, resid, gain, w_gate, w_up, w_down):
    groups = lax.axis_size("section") * lax.axis_size("rep")
    n_seq = lax.axis_size("seq")
    fits = (
        n_seq == SEQ
        and groups == 4
        and lax.axis_size("rep") == 2
        and wo.shape[1] % 128 == 0
        and (queries.shape[0] // groups) % 16 == 0
        and w_gate.shape[0] % 32 == 0
        and (queries.shape[0] * n_seq // groups) % 128 == 0
    )
    form = exchanged if fits else gathered
    return form(queries, keys, values, block_order, wo, resid, gain, w_gate, w_up, w_down)


def solution(mesh):
    return jax.shard_map(
        on_device,
        mesh=mesh,
        in_specs=(
            P("seq", ("section", "rep")),
            P("seq", ("section", "rep")),
            P("seq", ("section", "rep")),
            P(),
            P(("section", "rep"), "seq"),
            P(("section", "rep"), "seq", None),
            P("seq"),
            P("seq", None),
            P("seq", None),
            P("seq", None),
        ),
        out_specs=P(("section", "rep"), "seq", None),
        check_vma=False,
    )
```
